32 devices in a mesh: tm: 2 (over core), stn: 4 (over z), chan: 4 (over y, x).
Axes of the slice: x: 2, y: 2, z: 4, core: 2. Of those that a mesh axis runs over, the one named last changes fastest.
Arguments:
- voltages: bfloat16 [2, 8, 512, 32, 2, 256], P(None, 'chan', 'stn', 'tm'), may hold values from -100 to 100
- fir_taps: float32 [16, 256], replicated, may hold values from -1.5 to 1.5
- station_map: int32 [512], P('stn'), may hold values from 0 to 31, as said below
- beam_index: int32 [512], P('stn'), may hold values from 0 to 15
- weight_table: bfloat16 [2, 16, 8, 8], P(None, None, 'chan'), may hold values from -1.5 to 1.5
Outputs:
- visibilities: float32 [2, 2, 8, 32, 32, 8, 2, 2, 256], P('tm', None, 'chan', 'stn')
The draws below stay inside these ranges and needn't reach their ends.
Inputs may be any that keep to these rules, and one draw needn't show every extreme that they name: `station_map`: each station number names exactly 16 dishes; of the dishes g * 128 up to (g + 1) * 128 - 1, exactly 32 name a station of the block h * 8 up to (h + 1) * 8 - 1, for every g and h.
All inputs are finite; a program needn't handle non-finite values.
Results may differ from the reference program's by a relative error of at most 0.017.
Values may be sent and summed in bfloat16 or wider, within the bound.
A program may use at most 512 MiB of HBM per device.

```python
import jax
import jax.numpy as jnp
from jax import lax

DISHES = 512
STATIONS = 32
DPS = 16
BEAMS = 8
POL = 2
COARSE = 8
FINE = 256
TAPS = 16
NTAB = 16
FRAMES_DEV = 16
FRAMES = 32
N_TM = 2
N_STN = 4


def draw_voltages(key, part):
    noise_key, sample_key, frame_key = jax.random.split(jax.random.fold_in(key, 11), 3)
    shape = (2, COARSE, DISHES, FRAMES, POL, FINE)
    noise_draw = jnp.clip(jax.random.normal(noise_key, shape, jnp.float32), -6.0, 6.0)
    rise_factor = 3.0
    coarse_pos = jnp.arange(COARSE, dtype=jnp.float32) / max(COARSE - 1, 1)
    coarse_amp = jnp.sqrt(rise_factor ** coarse_pos)
    sample_amp = 10.0 ** (0.5 * jax.random.uniform(sample_key, (FINE,), jnp.float32))
    frame_amp = 3.0 ** (0.5 * jax.random.uniform(frame_key, (FRAMES,), jnp.float32))
    scaled = noise_draw * coarse_amp[None, :, None, None, None, None] * frame_amp[None, None, None, :, None, None] * sample_amp
    return scaled.astype(jnp.bfloat16)


def draw_station_map(key, part):
    group_dishes = DISHES // N_STN
    share = group_dishes // N_STN
    owned = STATIONS // N_STN
    first_key, second_key = jax.random.split(jax.random.fold_in(key, 23), 2)
    base = jnp.arange(group_dishes, dtype=jnp.int32)
    ranks = jax.vmap(lambda sub_key: jax.random.permutation(sub_key, base))(jax.random.split(first_key, N_STN))
    placing = jax.vmap(lambda sub_key: jax.random.permutation(sub_key, base))(jax.random.split(second_key, N_STN))
    owner = ranks // share
    group_ids = jnp.arange(N_STN, dtype=jnp.int32)[:, None]
    column = group_ids * share + ranks % share
    position = placing[owner, column]
    station = owner * owned + position // (DISHES // STATIONS)
    return station.reshape(DISHES).astype(jnp.int32)


def place_ends(values, stream_key, least, largest):
    dims = values.shape
    index_at = [jax.random.randint(jax.random.fold_in(stream_key, axis), (), 0, dims[axis]) for axis in range(len(dims))]
    values = values.at[tuple(index_at)].set(least)
    longest = dims.index(max(dims))
    index_at[longest] = (index_at[longest] + 1) % dims[longest]
    return values.at[tuple(index_at)].set(largest)


def level_of(key, shape, cuts, smallest, largest):
    def one(dim, blocks):
        heights = jax.random.uniform(jax.random.fold_in(jax.random.fold_in(key, 6), dim), (blocks,), jnp.float32, smallest / len(cuts), largest / len(cuts))
        return jnp.repeat(jnp.exp(heights), shape[dim] // blocks).reshape((-1,) + (1,) * (len(shape) - dim - 1))

    level = one(*cuts[0])
    for cut in cuts[1:]:
        level = level * one(*cut)
    return level


def bell_draw(rng, shape, deviation, most, pieces=(), kind=jnp.bfloat16):
    level = level_of(rng, shape, pieces, -0.22, 0.18) if pieces else 1.0
    array = jax.random.normal(rng, shape, jnp.float32) * deviation * level
    return jnp.minimum(jnp.maximum(array, -most), most).astype(kind)


def setup_inputs(seed: int = 0) -> dict:
    seeds = jax.random.split(jax.random.key(seed), 6)
    voltages = draw_voltages(jax.random.fold_in(seeds[5], 71), 0)
    fir_taps = bell_draw(seeds[1], (TAPS, FINE), TAPS ** -0.5, 1.5, (), jnp.float32)
    station_map = draw_station_map(jax.random.fold_in(seeds[5], 71), 0)
    beam_index = place_ends(jax.random.randint(seeds[3], (DISHES,), 0, NTAB), jax.random.fold_in(seeds[3], 1), 0, NTAB - 1).astype(jnp.int32)
    weight_table = bell_draw(seeds[4], (2, NTAB, COARSE, BEAMS), DPS ** -0.5, 1.5, ((2, 4),))
    return {"voltages": voltages, "fir_taps": fir_taps, "station_map": station_map, "beam_index": beam_index, "weight_table": weight_table}


epsilon = 1e-06

def dft_tables(length):
    bin_index = jnp.arange(length, dtype=jnp.int32)
    phase_step = bin_index[:, None] * bin_index[None, :] % length
    angles = phase_step.astype(jnp.float32) * (2.0 * jnp.pi / length)
    return (jnp.cos(angles).astype(jnp.bfloat16), jnp.sin(angles).astype(jnp.bfloat16))

def correlate(normed_slice):
    values = normed_slice.astype(jnp.float32)
    real_part = values[:, 0]
    imag_part = values[:, 1]

    def product(left_beams, right_beams):
        return jnp.einsum('sbfpk,tbfqk->stbpqk', left_beams, right_beams)
    vis_re = product(real_part, real_part) + product(imag_part, imag_part)
    vis_im = product(imag_part, real_part) - product(real_part, imag_part)
    return jnp.stack([vis_re, vis_im]) / FRAMES_DEV

def reference(voltages, fir_taps, station_map, beam_index, weight_table):
    cosine, sine_table = dft_tables(FINE)
    history = TAPS - 1
    group_size = DISHES // N_STN
    station_hot = (station_map[:, None] == jnp.arange(STATIONS, dtype=jnp.int32)[None, :]).astype(jnp.float32)
    table_hot = (beam_index[:, None] == jnp.arange(NTAB, dtype=jnp.int32)[None, :]).astype(jnp.float32)

    def channel_beams(inputs):
        samples, table_slice = inputs
        padded = jnp.pad(samples, ((0, 0), (0, 0), (history, 0), (0, 0), (0, 0)))
        filtered = jnp.zeros(samples.shape, jnp.float32)
        for tap_index in range(TAPS):
            offset = history - tap_index
            filtered = filtered + fir_taps[tap_index] * padded[:, :, offset:offset + FRAMES].astype(jnp.float32)
        filtered = filtered.astype(jnp.bfloat16)
        real_part = filtered[0].reshape(-1, FINE)
        imag_part = filtered[1].reshape(-1, FINE)
        spec_re = jnp.dot(real_part, cosine, preferred_element_type=jnp.float32) + jnp.dot(imag_part, sine_table, preferred_element_type=jnp.float32)
        spec_im = jnp.dot(imag_part, cosine, preferred_element_type=jnp.float32) - jnp.dot(real_part, sine_table, preferred_element_type=jnp.float32)
        spectra_low = jnp.stack([spec_re, spec_im]).reshape(samples.shape).astype(jnp.bfloat16)
        spectra = lax.optimization_barrier(spectra_low).astype(jnp.float32)
        weights = jnp.einsum('dt,otb->odb', table_hot, table_slice.astype(jnp.float32))
        weight_re = weights[0]
        weight_im = weights[1]
        mixing = jnp.stack([jnp.stack([weight_re, -weight_im]), jnp.stack([weight_im, weight_re])])
        steering = station_hot[None, None, :, :, None] * mixing[:, :, :, None, :]
        summed = jnp.zeros((STATIONS, 2, BEAMS, FRAMES, POL, FINE), jnp.float32)
        for dish_group in range(N_STN):
            low_dish = dish_group * group_size
            partial_value = jnp.einsum('oidsb,idfpk->sobfpk', steering[:, :, low_dish:low_dish + group_size], spectra[:, low_dish:low_dish + group_size])
            rounded = lax.optimization_barrier(partial_value.astype(jnp.bfloat16))
            summed = summed + rounded.astype(jnp.float32)
        return summed.astype(jnp.bfloat16)
    formed = lax.map(channel_beams, (jnp.moveaxis(voltages, 1, 0), jnp.moveaxis(weight_table, 2, 0)))
    outputs = []
    for time_block in range(N_TM):
        first_frame = time_block * FRAMES_DEV
        values = formed[:, :, :, :, first_frame:first_frame + FRAMES_DEV].astype(jnp.float32)
        power_sum = lax.optimization_barrier(jnp.sum(values * values, axis=(0, 2, 4, 6)))
        inverse_rms = lax.rsqrt(power_sum / (COARSE * FRAMES_DEV * FINE) + epsilon)
        normed = (values * inverse_rms[None, :, None, :, None, :, None]).astype(jnp.bfloat16)
        visibility = lax.map(correlate, normed)
        outputs.append(jnp.moveaxis(visibility, 0, 1))
    return jnp.stack(outputs)
```

```python
import functools

import jax
import jax.numpy as jnp
from jax import lax
from jax.experimental import pallas as pl
from jax.experimental.pallas import tpu as pltpu
from jax.sharding import PartitionSpec as P

LANES = 128
VMEM_LIMIT = 63 * 1024 * 1024
MESH = pl.DeviceIdType.MESH

epsilon = 1e-06


def dft_table(length):
    bin_index = jnp.arange(length, dtype=jnp.int32)
    phase_step = bin_index[:, None] * bin_index[None, :] % length
    angles = phase_step.astype(jnp.float32) * (2.0 * jnp.pi / length)
    cosine = jnp.cos(angles).astype(jnp.bfloat16)
    sine = jnp.sin(angles).astype(jnp.bfloat16)
    top = jnp.concatenate([cosine, -sine], axis=1)
    return jnp.concatenate([top, jnp.concatenate([sine, cosine], axis=1)], axis=0)


def chain_kernel(
    beams, volts, perm, steer, taps, dft, out,
    xin, send, recv, srecv, sfull, ybuf, fil, gbuf, pacc, pwx, scales, left, right, stage,
    load_sem, a_send, a_recv, s_send, s_recv, h_send, h_recv,
    b_send, b_recv, p_send, p_recv, c_send, c_recv, o_sem,
):
    coarse, polars, frames, _, dishes, fine = volts.shape
    chunks = coarse * polars
    n_taps = taps.shape[0]
    history = n_taps - 1
    n = lax.axis_size("stn")
    n_tm = lax.axis_size("tm")
    n_chan = lax.axis_size("chan")
    me = lax.axis_index("stn")
    tm = lax.axis_index("tm")
    ch = lax.axis_index("chan")
    share = dishes // n
    rows = sfull.shape[1]
    half_rows = rows // 2
    own = half_rows // beams
    halves = fine // LANES
    group = 4

    barrier = pltpu.get_barrier_semaphore()
    for k in range(1, n):
        pl.semaphore_signal(
            barrier, inc=1, device_id={"stn": lax.rem(me + k, n)}, device_id_type=MESH
        )
    for k in range(1, n_chan):
        pl.semaphore_signal(
            barrier, inc=1, device_id={"chan": lax.rem(ch + k, n_chan)}, device_id_type=MESH
        )
    for k in range(1, n_tm):
        pl.semaphore_signal(
            barrier, inc=1, device_id={"tm": lax.rem(tm + k, n_tm)}, device_id_type=MESH
        )

    def load(chunk):
        return pltpu.make_async_copy(
            volts.at[chunk // polars, chunk % polars],
            xin.at[chunk % 2],
            load_sem.at[chunk % 2],
        )

    def steer_copy(k):
        dest = lax.rem(me + k, n)
        return pltpu.make_async_remote_copy(
            src_ref=steer.at[dest], dst_ref=srecv.at[me],
            send_sem=s_send.at[k - 1], recv_sem=s_recv.at[k - 1],
            device_id={"stn": dest}, device_id_type=MESH,
        )

    def steer_arrival(k):
        return pltpu.make_async_remote_copy(
            src_ref=steer.at[me], dst_ref=srecv.at[lax.rem(me + n - k, n)],
            send_sem=s_send.at[k - 1], recv_sem=s_recv.at[k - 1],
            device_id={"stn": lax.rem(me + k, n)}, device_id_type=MESH,
        )

    def dish_copy(chunk, k):
        dest = lax.rem(me + k, n)
        return pltpu.make_async_remote_copy(
            src_ref=send.at[chunk, dest], dst_ref=recv.at[chunk, me],
            send_sem=a_send.at[chunk, k - 1], recv_sem=a_recv.at[chunk, k - 1],
            device_id={"stn": dest}, device_id_type=MESH,
        )

    def dish_arrival(chunk, k):
        return pltpu.make_async_remote_copy(
            src_ref=send.at[chunk, me], dst_ref=recv.at[chunk, lax.rem(me + n - k, n)],
            send_sem=a_send.at[chunk, k - 1], recv_sem=a_recv.at[chunk, k - 1],
            device_id={"stn": lax.rem(me + k, n)}, device_id_type=MESH,
        )

    load(0).start()
    srecv[me] = steer[me]

    for chunk in range(chunks):
        load(chunk).wait()
        if chunk + 1 < chunks:
            load(chunk + 1).start()

        def sort_step(i, carry):
            frame = i // 2
            o = i % 2
            moved = jnp.dot(
                perm[...], xin[chunk % 2, frame, o], preferred_element_type=jnp.float32
            ).astype(jnp.bfloat16)
            for dest in range(n):
                send[chunk, dest, frame, o] = moved[dest * share : (dest + 1) * share]
            return carry

        lax.fori_loop(0, 2 * frames, sort_step, 0)
        if chunk == 0:
            pl.semaphore_wait(barrier, (n - 1) + (n_chan - 1) + (n_tm - 1))
            for k in range(1, n):
                steer_copy(k).start()
        for k in range(1, n):
            dish_copy(chunk, k).start()

    def keep_step(i, carry):
        for chunk in range(chunks):
            recv[chunk, me, i] = send[chunk, me, i]
        return carry

    lax.fori_loop(0, frames, keep_step, 0)

    @pl.when(tm == 0)
    def _():
        def zero_step(i, carry):
            for chunk in range(chunks):
                ybuf[chunk, i] = jnp.zeros((rows, fine), jnp.bfloat16)
            return carry

        lax.fori_loop(0, history, zero_step, 0)

    pacc[...] = jnp.zeros_like(pacc)

    for k in range(1, n):
        steer_arrival(k).wait_recv()
    for c in range(coarse):
        columns = srecv[:, c].astype(jnp.float32).reshape(n * 2 * share, rows)
        sfull[c] = jnp.transpose(columns).astype(jnp.bfloat16)

    def halo(chunk):
        return pltpu.make_async_remote_copy(
            src_ref=ybuf.at[chunk, pl.ds(frames, history)],
            dst_ref=ybuf.at[chunk, pl.ds(0, history)],
            send_sem=h_send.at[chunk], recv_sem=h_recv.at[chunk],
            device_id={"tm": lax.rem(tm + 1, n_tm)}, device_id_type=MESH,
        )

    def beam_copy(block, chunk, right_way, distance):
        target = me + 1 if right_way else me - 1
        way = 0 if right_way else 1
        return pltpu.make_async_remote_copy(
            src_ref=gbuf.at[block, chunk], dst_ref=gbuf.at[block, chunk],
            send_sem=b_send.at[way, distance, chunk], recv_sem=b_recv.at[way, distance, chunk],
            device_id={"stn": lax.rem(target + n, n)}, device_id_type=MESH,
        )

    def chunk_work(chunk):
        c, p = chunk // polars, chunk % polars
        for k in range(1, n):
            dish_arrival(chunk, k).wait_recv()

        def beam_step(frame, carry):
            terms = recv[chunk, :, frame]
            if share % 16:
                terms = terms.astype(jnp.float32).reshape(-1, fine).astype(jnp.bfloat16)
            else:
                terms = terms.reshape(-1, fine)
            formed = jnp.dot(sfull[c], terms, preferred_element_type=jnp.float32)
            ybuf[chunk, history + frame] = formed.astype(jnp.bfloat16)
            return carry

        lax.fori_loop(0, frames, beam_step, 0)

        @pl.when(tm < n_tm - 1)
        def _():
            halo(chunk).start()

        @pl.when(tm > 0)
        def _():
            halo(chunk).wait_recv()

        part = min(32, half_rows)

        def filter_step(i, carry):
            for j in range(group):
                frame = i * group + j
                for o in range(2):
                    for low in range(0, half_rows, part):
                        start = o * half_rows + low
                        total = jnp.zeros((part, fine), jnp.float32)
                        for tap in range(n_taps):
                            sample = ybuf[chunk, frame + (history - tap), start : start + part, :]
                            total = total + taps[tap : tap + 1, :] * sample.astype(jnp.float32)
                        fil[
                            j * half_rows + low : j * half_rows + low + part,
                            o * fine : (o + 1) * fine,
                        ] = total.astype(jnp.bfloat16)
            spec = jnp.dot(fil[...], dft[...], preferred_element_type=jnp.float32)
            spec = spec.astype(jnp.bfloat16)
            for j in range(group):
                for o in range(2):
                    values = spec[j * half_rows : (j + 1) * half_rows, o * fine : (o + 1) * fine]
                    gbuf[me, chunk, i * group + j, o * half_rows : (o + 1) * half_rows, :] = values
                    wide = values.astype(jnp.float32)
                    pacc[p] += wide * wide
            return carry

        lax.fori_loop(0, frames // group, filter_step, 0)

        @pl.when(me < n - 1)
        def _():
            beam_copy(me, chunk, True, 0).start()

        @pl.when(me > 0)
        def _():
            beam_copy(me, chunk, False, 0).start()

    inner = jnp.logical_and(me > 0, me < n - 1)

    def from_side(block, chunk, right_way, distance, forward):
        beam_copy(block, chunk, right_way, distance).wait_recv()
        if forward:
            beam_copy(block, chunk, right_way, distance + 1).start()

    def pass_on(distance, chunk):
        @pl.when(inner)
        def _():
            @pl.when(me - distance >= 0)
            def _():
                from_side(me - distance, chunk, True, distance - 1, True)

            @pl.when(me + distance < n)
            def _():
                from_side(me + distance, chunk, False, distance - 1, True)

    def arrive(distance, chunk):
        @pl.when(me == n - 1)
        def _():
            from_side(me - distance, chunk, True, distance - 1, False)

        @pl.when(me == 0)
        def _():
            from_side(me + distance, chunk, False, distance - 1, False)

    def power_copy(k):
        return pltpu.make_async_remote_copy(
            src_ref=pwx.at[ch], dst_ref=pwx.at[ch],
            send_sem=p_send.at[k - 1], recv_sem=p_recv.at[k - 1],
            device_id={"chan": lax.rem(ch + k, n_chan)}, device_id_type=MESH,
        )

    def power_arrival(k):
        other = lax.rem(ch + n_chan - k, n_chan)
        return pltpu.make_async_remote_copy(
            src_ref=pwx.at[ch], dst_ref=pwx.at[other],
            send_sem=p_send.at[k - 1], recv_sem=p_recv.at[k - 1],
            device_id={"chan": lax.rem(ch + k, n_chan)}, device_id_type=MESH,
        )

    def scale_copy(k):
        return pltpu.make_async_remote_copy(
            src_ref=scales.at[me], dst_ref=scales.at[me],
            send_sem=c_send.at[k - 1], recv_sem=c_recv.at[k - 1],
            device_id={"stn": lax.rem(me + k, n)}, device_id_type=MESH,
        )

    def scale_arrival(k):
        other = lax.rem(me + n - k, n)
        return pltpu.make_async_remote_copy(
            src_ref=scales.at[me], dst_ref=scales.at[other],
            send_sem=c_send.at[k - 1], recv_sem=c_recv.at[k - 1],
            device_id={"stn": lax.rem(me + k, n)}, device_id_type=MESH,
        )

    def power_work():
        for p in range(polars):
            total = jnp.sum(pacc[p], axis=1, keepdims=True)
            pwx[ch, p] = jnp.broadcast_to(total, (half_rows, LANES))
        for k in range(1, n_chan):
            power_copy(k).start()
        for k in range(1, n_chan):
            power_arrival(k).wait_recv()
        total = pwx[0]
        for k in range(1, n_chan):
            total = total + pwx[k]
        scales[me] = lax.rsqrt(total / (coarse * n_chan * frames * fine) + epsilon)
        for k in range(1, n):
            scale_copy(k).start()
        for k in range(1, n):
            scale_arrival(k).wait_recv()

    def widen(block, c, target):
        def step(i, carry):
            for p in range(polars):
                target[p, i] = gbuf[block, c * polars + p, i].astype(jnp.float32)
            return carry

        lax.fori_loop(0, frames, step, 0)

    def out_copy(slot, c, s, block):
        return pltpu.make_async_copy(
            stage.at[slot], out.at[:, c, s, pl.ds(block * own, own)], o_sem.at[slot]
        )

    def correlate(c, block, first):
        widen(block, c, right)

        def station(s, carry):
            slot = s % 2
            srow = pl.multiple_of(s * beams, beams)
            if first:
                @pl.when(s >= 2)
                def _():
                    out_copy(slot, c, s, block).wait()
            else:
                out_copy(slot, c, s, block).wait()

            def pair(t, inner_carry):
                trow = pl.multiple_of(t * beams, beams)
                for half in range(halves):
                    lanes = pl.ds(half * LANES, LANES)
                    re = {}
                    im = {}
                    for f in range(frames):
                        lre = [left[p, f, pl.ds(srow, beams), lanes] for p in range(polars)]
                        lim = [
                            left[p, f, pl.ds(half_rows + srow, beams), lanes]
                            for p in range(polars)
                        ]
                        rre = [right[q, f, pl.ds(trow, beams), lanes] for q in range(polars)]
                        rim = [
                            right[q, f, pl.ds(half_rows + trow, beams), lanes]
                            for q in range(polars)
                        ]
                        for p in range(polars):
                            for q in range(polars):
                                a = lre[p] * rre[q] + lim[p] * rim[q]
                                b = lim[p] * rre[q] - lre[p] * rim[q]
                                re[p, q] = a if f == 0 else re[p, q] + a
                                im[p, q] = b if f == 0 else im[p, q] + b
                    for p in range(polars):
                        for q in range(polars):
                            scale = (
                                scales[me, p, pl.ds(srow, beams), :]
                                * scales[block, q, pl.ds(trow, beams), :]
                                * (1.0 / frames)
                            )
                            row = (p * halves + half) * polars + q
                            where = pl.ds(row, beams, stride=polars * polars * halves)
                            stage[slot, 0, t, where, :] = re[p, q] * scale
                            stage[slot, 1, t, where, :] = im[p, q] * scale
                return inner_carry

            lax.fori_loop(0, own, pair, 0)
            out_copy(slot, c, s, block).start()
            return carry

        lax.fori_loop(0, own, station, 0)

    def order(step):
        if step == 0:
            return me
        two_sided = jnp.minimum(me, n - 1 - me)
        near = (step + 1) // 2
        near_block = me - near if step % 2 else me + near
        far = step - two_sided
        far_block = jnp.where(me < n - 1 - me, me + far, me - far)
        return jnp.where(step <= 2 * two_sided, near_block, far_block)

    for chunk in range(polars):
        chunk_work(chunk)
    for c in range(1, coarse):
        for p in range(polars):
            chunk_work(c * polars + p)
            for q in range(polars):
                if p == 0:
                    pass_on(1, (c - 1) * polars + q)
        for distance in range(2, n - 1):
            for q in range(polars):
                pass_on(distance, (c - 1) * polars + q)
    power_work()
    widen(me, 0, left)
    last = coarse - 1
    for c in range(coarse):
        if c:
            widen(me, c, left)
        for step in range(n):
            if step >= 1:
                for q in range(polars):
                    arrive(step, c * polars + q)
            if c == last and coarse == 1 and step == 0:
                for distance in range(1, n - 1):
                    for q in range(polars):
                        pass_on(distance, c * polars + q)
            correlate(c, order(step), c == 0 and step == 0)
            if c == last - 1 and step >= n - 2:
                for q in range(polars):
                    if step == n - 2:
                        pass_on(1, last * polars + q)
            if c == last - 1 and step == n - 1:
                for distance in range(2, n - 1):
                    for q in range(polars):
                        pass_on(distance, last * polars + q)

    for slot in range(2):
        out_copy(slot, last, own - 2 + slot, order(n - 1)).wait()
    for k in range(1, n):
        steer_copy(k).wait_send()
        scale_copy(k).wait_send()
        for chunk in range(chunks):
            dish_copy(chunk, k).wait_send()
    for k in range(1, n_chan):
        power_copy(k).wait_send()

    @pl.when(tm < n_tm - 1)
    def _():
        for chunk in range(chunks):
            halo(chunk).wait_send()

    for distance in range(n - 1):
        for chunk in range(chunks):
            @pl.when(jnp.logical_and(me - distance >= 0, me < n - 1))
            def _():
                beam_copy(me - distance, chunk, True, distance).wait_send()

            @pl.when(jnp.logical_and(me + distance < n, me > 0))
            def _():
                beam_copy(me + distance, chunk, False, distance).wait_send()


def chain(volts, perm, steer, fir_taps, table, beams):
    coarse, polars, frames, _, dishes, fine = volts.shape
    n, _, terms, rows = steer.shape
    n_chan = lax.axis_size("chan")
    share = dishes // n
    chunks = coarse * polars
    half_rows = rows // 2
    own = half_rows // beams
    out_rows = beams * polars * polars * (fine // LANES)
    history = fir_taps.shape[0] - 1
    dma = pltpu.SemaphoreType.DMA
    bf16, f32 = jnp.bfloat16, jnp.float32
    size = 2 * coarse * own * n * own * out_rows * LANES
    vmem = pl.BlockSpec(memory_space=pltpu.VMEM)
    return pl.pallas_call(
        functools.partial(chain_kernel, beams),
        in_specs=[pl.BlockSpec(memory_space=pl.ANY), vmem, vmem, vmem, vmem],
        out_specs=pl.BlockSpec(memory_space=pl.ANY),
        out_shape=jax.ShapeDtypeStruct((2, coarse, own, n * own, out_rows, LANES), f32),
        scratch_shapes=[
            pltpu.VMEM((2, frames, 2, dishes, fine), bf16),
            pltpu.VMEM((chunks, n, frames, 2, share, fine), bf16),
            pltpu.VMEM((chunks, n, frames, 2, share, fine), bf16),
            pltpu.VMEM((n, coarse, terms, rows), bf16),
            pltpu.VMEM((coarse, rows, n * terms), bf16),
            pltpu.VMEM((chunks, history + frames, rows, fine), bf16),
            pltpu.VMEM((4 * half_rows, 2 * fine), bf16),
            pltpu.VMEM((n, chunks, frames, rows, fine), bf16),
            pltpu.VMEM((polars, half_rows, fine), f32),
            pltpu.VMEM((n_chan, polars, half_rows, LANES), f32),
            pltpu.VMEM((n, polars, half_rows, LANES), f32),
            pltpu.VMEM((polars, frames, rows, fine), f32),
            pltpu.VMEM((polars, frames, rows, fine), f32),
            pltpu.VMEM((2, 2, own, out_rows, LANES), f32),
            dma((2,)),
            dma((chunks, n - 1)),
            dma((chunks, n - 1)),
            dma((n - 1,)),
            dma((n - 1,)),
            dma((chunks,)),
            dma((chunks,)),
            dma((2, n - 1, chunks)),
            dma((2, n - 1, chunks)),
            dma((n_chan - 1,)),
            dma((n_chan - 1,)),
            dma((n - 1,)),
            dma((n - 1,)),
            dma((2,)),
        ],
        compiler_params=pltpu.CompilerParams(
            vmem_limit_bytes=VMEM_LIMIT, collective_id=0, has_side_effects=True
        ),
        cost_estimate=pl.CostEstimate(
            flops=size * 4 * frames * 100, bytes_accessed=size * 4, transcendentals=0
        ),
        name="chain",
    )(volts, perm, steer, fir_taps, table)


def per_device(voltages, fir_taps, station_map, beam_index, weight_table):
    _, coarse_dev, dishes, frames, polars, fine = voltages.shape
    table_rows, beams = weight_table.shape[1], weight_table.shape[3]
    n = lax.axis_size("stn")
    share = dishes // n
    total_stations = 32
    own = total_stations // n
    order = jnp.arange(dishes, dtype=jnp.int32)
    block = station_map // own
    same = block[:, None] == block[None, :]
    before = order[None, :] < order[:, None]
    rank = jnp.sum((same & before).astype(jnp.int32), axis=1)
    place = block * share + rank
    hot = place[None, :] == order[:, None]
    perm = hot.astype(jnp.bfloat16)
    station = jnp.sum(jnp.where(hot, (station_map - block * own)[None, :], 0), axis=1)
    row = jnp.sum(jnp.where(hot, beam_index[None, :], 0), axis=1)
    station_hot = station[:, None] == jnp.arange(own, dtype=jnp.int32)
    table_hot = (row[:, None] == jnp.arange(table_rows, dtype=jnp.int32)).astype(jnp.bfloat16)
    weights = jnp.einsum(
        "dt,otcb->ocdb", table_hot, weight_table, preferred_element_type=jnp.float32
    ).astype(jnp.bfloat16)
    mixing = jnp.stack(
        [jnp.stack([weights[0], weights[1]]), jnp.stack([-weights[1], weights[0]])]
    )
    mixing = mixing.reshape(2, 2, coarse_dev, n, share, 1, beams)
    steer = jnp.where(
        station_hot.reshape(1, 1, 1, n, share, own, 1), mixing, jnp.zeros((), jnp.bfloat16)
    )
    steer = jnp.transpose(steer, (3, 2, 0, 4, 1, 5, 6))
    steer = steer.reshape(n, coarse_dev, 2 * share, 2 * own * beams)
    volts = jnp.transpose(voltages, (1, 4, 3, 0, 2, 5))
    result = chain(volts, perm, steer, fir_taps, dft_table(fine), beams)
    halves = fine // LANES
    result = result.reshape(
        2, coarse_dev, own, total_stations, beams, polars, halves, polars, LANES
    )
    result = jnp.swapaxes(result, 6, 7)
    return result.reshape(1, 2, coarse_dev, own, total_stations, beams, polars, polars, fine)


def solution(mesh):
    in_specs = (
        P(None, "chan", "stn", "tm", None, None),
        P(),
        P("stn"),
        P("stn"),
        P(None, None, "chan", None),
    )
    out_specs = P("tm", None, "chan", "stn", None, None, None, None, None)
    return jax.shard_map(
        per_device, mesh=mesh, in_specs=in_specs, out_specs=out_specs, check_vma=False
    )
```

```python
import functools

import jax
import jax.numpy as jnp
import numpy as np
from jax import lax
from jax.experimental import pallas as pl
from jax.experimental.pallas import tpu as pltpu
from jax.sharding import PartitionSpec as P

LANES = 128
VMEM_LIMIT = 63 * 1024 * 1024
MESH = pl.DeviceIdType.MESH

epsilon = 1e-06


def dft_table(length):
    bin_index = np.arange(length)
    phase_step = bin_index[:, None] * bin_index[None, :] % length
    angles = (2.0 * np.pi / length) * phase_step
    cosine = np.cos(angles)
    sine = np.sin(angles)
    table = np.block([[cosine, -sine], [sine, cosine]])
    return jnp.asarray(table.astype(np.float32), jnp.bfloat16)


def chain_kernel(
    beams, volts, perm, steer, taps, dft, out, lout, rout,
    xin, send, recv, srecv, sfull, ybuf, fil, gbuf, pacc, pwx, scales, lrows, rrows, left, right, stage,
    load_sem, a_send, a_recv, s_send, s_recv, h_send, h_recv,
    b_send, b_recv, p_send, p_recv, c_send, c_recv, o_sem, r_sem,
):
    coarse, polars, frames, _, dishes, fine = volts.shape
    chunks = coarse * polars
    n_taps = taps.shape[0]
    history = n_taps - 1
    n = lax.axis_size("stn")
    n_tm = lax.axis_size("tm")
    n_chan = lax.axis_size("chan")
    me = lax.axis_index("stn")
    tm = lax.axis_index("tm")
    ch = lax.axis_index("chan")
    share = dishes // n
    rows = sfull.shape[1]
    half_rows = rows // 2
    own = half_rows // beams
    halves = fine // LANES
    group = 4
    unroll = 8
    ahead = 2

    barrier = pltpu.get_barrier_semaphore()
    for k in range(1, n):
        pl.semaphore_signal(
            barrier, inc=1, device_id={"stn": lax.rem(me + k, n)}, device_id_type=MESH
        )
    for k in range(1, n_chan):
        pl.semaphore_signal(
            barrier, inc=1, device_id={"chan": lax.rem(ch + k, n_chan)}, device_id_type=MESH
        )
    for k in range(1, n_tm):
        pl.semaphore_signal(
            barrier, inc=1, device_id={"tm": lax.rem(tm + k, n_tm)}, device_id_type=MESH
        )

    def load(chunk):
        return pltpu.make_async_copy(
            volts.at[chunk // polars, chunk % polars],
            xin.at[chunk % 2],
            load_sem.at[chunk % 2],
        )

    def steer_copy(k):
        dest = lax.rem(me + k, n)
        return pltpu.make_async_remote_copy(
            src_ref=steer.at[dest], dst_ref=srecv.at[me],
            send_sem=s_send.at[k - 1], recv_sem=s_recv.at[k - 1],
            device_id={"stn": dest}, device_id_type=MESH,
        )

    def steer_arrival(k):
        return pltpu.make_async_remote_copy(
            src_ref=steer.at[me], dst_ref=srecv.at[lax.rem(me + n - k, n)],
            send_sem=s_send.at[k - 1], recv_sem=s_recv.at[k - 1],
            device_id={"stn": lax.rem(me + k, n)}, device_id_type=MESH,
        )

    def dish_copy(chunk, k):
        dest = lax.rem(me + k, n)
        return pltpu.make_async_remote_copy(
            src_ref=send.at[chunk, dest], dst_ref=recv.at[chunk, me],
            send_sem=a_send.at[chunk, k - 1], recv_sem=a_recv.at[chunk, k - 1],
            device_id={"stn": dest}, device_id_type=MESH,
        )

    def dish_arrival(chunk, k):
        return pltpu.make_async_remote_copy(
            src_ref=send.at[chunk, me], dst_ref=recv.at[chunk, lax.rem(me + n - k, n)],
            send_sem=a_send.at[chunk, k - 1], recv_sem=a_recv.at[chunk, k - 1],
            device_id={"stn": lax.rem(me + k, n)}, device_id_type=MESH,
        )

    def send_dishes(chunk):
        for distance in range(1, n):
            @pl.when(me + distance < n)
            def _():
                dish_copy(chunk, distance).start()

            @pl.when(me - distance >= 0)
            def _():
                dish_copy(chunk, n - distance).start()

    load(0).start()
    srecv[me] = steer[me]

    for chunk in range(chunks):
        load(chunk).wait()
        if chunk + 1 < chunks:
            load(chunk + 1).start()

        def sort_step(i, carry):
            frame = i // 2
            o = i % 2
            moved = jnp.dot(
                perm[...], xin[chunk % 2, frame, o], preferred_element_type=jnp.float32
            ).astype(jnp.bfloat16)
            for dest in range(n):
                send[chunk, dest, frame, o] = moved[dest * share : (dest + 1) * share]
            return carry

        lax.fori_loop(0, 2 * frames, sort_step, 0)
        if chunk == 0:
            pl.semaphore_wait(barrier, (n - 1) + (n_chan - 1) + (n_tm - 1))
            for k in range(1, n):
                steer_copy(k).start()
        if chunk < ahead:
            send_dishes(chunk)

    def keep_step(i, carry):
        for chunk in range(chunks):
            recv[chunk, me, i] = send[chunk, me, i]
        return carry

    lax.fori_loop(0, frames, keep_step, 0)

    @pl.when(tm == 0)
    def _():
        def zero_step(i, carry):
            for chunk in range(chunks):
                ybuf[chunk, i] = jnp.zeros((rows, fine), jnp.bfloat16)
            return carry

        lax.fori_loop(0, history, zero_step, 0)

    pacc[...] = jnp.zeros_like(pacc)

    for k in range(1, n):
        steer_arrival(k).wait_recv()
    for c in range(coarse):
        columns = srecv[:, c].astype(jnp.float32).reshape(n * 2 * share, rows)
        sfull[c] = jnp.transpose(columns).astype(jnp.bfloat16)

    def halo(chunk):
        return pltpu.make_async_remote_copy(
            src_ref=ybuf.at[chunk, pl.ds(frames, history)],
            dst_ref=ybuf.at[chunk, pl.ds(0, history)],
            send_sem=h_send.at[chunk], recv_sem=h_recv.at[chunk],
            device_id={"tm": lax.rem(tm + 1, n_tm)}, device_id_type=MESH,
        )

    def beam_copy(block, chunk, right_way, distance):
        target = me + 1 if right_way else me - 1
        way = 0 if right_way else 1
        return pltpu.make_async_remote_copy(
            src_ref=gbuf.at[block, chunk], dst_ref=gbuf.at[block, chunk],
            send_sem=b_send.at[way, distance, chunk], recv_sem=b_recv.at[way, distance, chunk],
            device_id={"stn": lax.rem(target + n, n)}, device_id_type=MESH,
        )

    inner = jnp.logical_and(me > 0, me < n - 1)
    low_side = me < n - 1 - me

    def on_side(far_way, distance, chunk, hop, act):
        for right_way in (True, False):
            block = me - distance if right_way else me + distance
            inside = block >= 0 if right_way else block < n
            side = low_side if right_way == far_way else jnp.logical_not(low_side)

            @pl.when(jnp.logical_and(jnp.logical_and(inner, side), inside))
            def _():
                act(beam_copy(block, chunk, right_way, hop))

    outward = (True, 2, [])
    inward_end = (False, 5, [])

    def launch(queue, distance, chunk):
        far_way, window, started = queue
        if len(started) >= window:
            past, past_chunk = started[-window]
            on_side(far_way, past, past_chunk, past, lambda copy: copy.wait_send())
        started.append((distance, chunk))
        on_side(far_way, distance, chunk, distance, lambda copy: copy.start())

    def receive(queue, distance, chunk):
        on_side(queue[0], distance, chunk, distance - 1, lambda copy: copy.wait_recv())

    def drain(queue):
        far_way, window, started = queue
        for distance, chunk in started[-window:]:
            on_side(far_way, distance, chunk, distance, lambda copy: copy.wait_send())

    def chunk_work(chunk):
        c, p = chunk // polars, chunk % polars
        for k in range(1, n):
            dish_arrival(chunk, k).wait_recv()
        if chunk + ahead < chunks:
            send_dishes(chunk + ahead)

        def beam_step(frame, carry):
            terms = recv[chunk, :, frame]
            if share % 16:
                terms = terms.astype(jnp.float32).reshape(-1, fine).astype(jnp.bfloat16)
            else:
                terms = terms.reshape(-1, fine)
            formed = jnp.dot(sfull[c], terms, preferred_element_type=jnp.float32)
            ybuf[chunk, history + frame] = formed.astype(jnp.bfloat16)
            return carry

        lax.fori_loop(0, frames, beam_step, 0)

        @pl.when(tm < n_tm - 1)
        def _():
            halo(chunk).start()

        @pl.when(tm > 0)
        def _():
            halo(chunk).wait_recv()

        part = min(32, half_rows)

        def filter_step(i, carry):
            for j in range(group):
                frame = i * group + j
                for o in range(2):
                    for low in range(0, half_rows, part):
                        start = o * half_rows + low
                        total = jnp.zeros((part, fine), jnp.float32)
                        for tap in range(n_taps):
                            sample = ybuf[chunk, frame + (history - tap), start : start + part, :]
                            total = total + taps[tap : tap + 1, :] * sample.astype(jnp.float32)
                        fil[
                            j * half_rows + low : j * half_rows + low + part,
                            o * fine : (o + 1) * fine,
                        ] = total.astype(jnp.bfloat16)
            spec = jnp.dot(fil[...], dft[...], preferred_element_type=jnp.float32)
            spec = spec.astype(jnp.bfloat16)
            for j in range(group):
                for o in range(2):
                    values = spec[j * half_rows : (j + 1) * half_rows, o * fine : (o + 1) * fine]
                    gbuf[me, chunk, i * group + j, o * half_rows : (o + 1) * half_rows, :] = values
                    wide = values.astype(jnp.float32)
                    pacc[p] += wide * wide
            return carry

        lax.fori_loop(0, frames // group, filter_step, 0)

        @pl.when(me == 0)
        def _():
            beam_copy(me, chunk, True, 0).start()

        @pl.when(me == n - 1)
        def _():
            beam_copy(me, chunk, False, 0).start()

        launch(inward_end, 0, chunk)

    def arrive(distance, chunk):
        @pl.when(me == n - 1)
        def _():
            beam_copy(me - distance, chunk, True, distance - 1).wait_recv()

        @pl.when(me == 0)
        def _():
            beam_copy(me + distance, chunk, False, distance - 1).wait_recv()

    def power_copy(k):
        return pltpu.make_async_remote_copy(
            src_ref=pwx.at[ch], dst_ref=pwx.at[ch],
            send_sem=p_send.at[k - 1], recv_sem=p_recv.at[k - 1],
            device_id={"chan": lax.rem(ch + k, n_chan)}, device_id_type=MESH,
        )

    def power_arrival(k):
        other = lax.rem(ch + n_chan - k, n_chan)
        return pltpu.make_async_remote_copy(
            src_ref=pwx.at[ch], dst_ref=pwx.at[other],
            send_sem=p_send.at[k - 1], recv_sem=p_recv.at[k - 1],
            device_id={"chan": lax.rem(ch + k, n_chan)}, device_id_type=MESH,
        )

    def scale_copy(k):
        return pltpu.make_async_remote_copy(
            src_ref=scales.at[me], dst_ref=scales.at[me],
            send_sem=c_send.at[k - 1], recv_sem=c_recv.at[k - 1],
            device_id={"stn": lax.rem(me + k, n)}, device_id_type=MESH,
        )

    def scale_arrival(k):
        other = lax.rem(me + n - k, n)
        return pltpu.make_async_remote_copy(
            src_ref=scales.at[me], dst_ref=scales.at[other],
            send_sem=c_send.at[k - 1], recv_sem=c_recv.at[k - 1],
            device_id={"stn": lax.rem(me + k, n)}, device_id_type=MESH,
        )

    def power_start():
        for p in range(polars):
            total = jnp.sum(pacc[p], axis=1, keepdims=True)
            pwx[ch, p] = jnp.broadcast_to(total, (half_rows, LANES))
        for k in range(1, n_chan):
            power_copy(k).start()

    def power_finish():
        for k in range(1, n_chan):
            power_arrival(k).wait_recv()
        total = pwx[0]
        for k in range(1, n_chan):
            total = total + pwx[k]
        scales[me] = lax.rsqrt(total / (coarse * n_chan * frames * fine) + epsilon)
        for k in range(1, n):
            scale_copy(k).start()

    def row_copies():
        return (
            pltpu.make_async_copy(lrows, lout, r_sem.at[0]),
            pltpu.make_async_copy(rrows, rout, r_sem.at[1]),
        )

    def scale_rows():
        for k in range(1, n):
            scale_arrival(k).wait_recv()

        def spread(t, target, by_left, block):
            row = pl.multiple_of(lax.rem(t, own) * beams, beams)
            for p in range(polars):
                for half in range(halves):
                    for q in range(polars):
                        where = pl.ds(
                            (p * halves + half) * polars + q, beams,
                            stride=polars * polars * halves,
                        )
                        value = scales[block, p if by_left else q, pl.ds(row, beams), :]
                        target[t, where, :] = value * (1.0 / frames) if by_left else value

        def left_step(t, carry):
            spread(t, lrows, True, me)
            return carry

        def right_step(t, carry):
            spread(t, rrows, False, t // own)
            return carry

        lax.fori_loop(0, own, left_step, 0)
        lax.fori_loop(0, n * own, right_step, 0)
        for copy in row_copies():
            copy.start()

    def widen(block, c, target):
        def step(i, carry):
            for p in range(polars):
                target[p, i] = gbuf[block, c * polars + p, i].astype(jnp.float32)
            return carry

        lax.fori_loop(0, frames, step, 0)

    def out_copy(slot, c, s, block):
        return pltpu.make_async_copy(
            stage.at[slot], out.at[:, c, s, pl.ds(block * (own // 2), own // 2)], o_sem.at[slot]
        )

    def correlate(c, block, first):
        widen(block, c, right)

        def station(s, carry):
            slot = s % 2
            srow = pl.multiple_of(s * beams, beams)
            if first:
                @pl.when(s >= 2)
                def _():
                    out_copy(slot, c, s, block).wait()
            else:
                out_copy(slot, c, s, block).wait()

            def pair(i, inner_carry):
                half = i % halves
                t = i // halves
                lanes = pl.ds(pl.multiple_of(half * LANES, LANES), LANES)
                trows = [pl.multiple_of((2 * t + x) * beams, beams) for x in range(2)]

                def some_frames(k, totals):
                    totals = list(totals)
                    for j in range(unroll):
                        f = k * unroll + j
                        lre = [left[p, f, pl.ds(srow, beams), lanes] for p in range(polars)]
                        lim = [
                            left[p, f, pl.ds(half_rows + srow, beams), lanes]
                            for p in range(polars)
                        ]
                        for x in range(2):
                            rre = [
                                right[q, f, pl.ds(trows[x], beams), lanes] for q in range(polars)
                            ]
                            rim = [
                                right[q, f, pl.ds(half_rows + trows[x], beams), lanes]
                                for q in range(polars)
                            ]
                            for p in range(polars):
                                for q in range(polars):
                                    at = ((x * polars + p) * polars + q) * 2
                                    totals[at] += lre[p] * rre[q] + lim[p] * rim[q]
                                    totals[at + 1] += lim[p] * rre[q] - lre[p] * rim[q]
                    return tuple(totals)

                zero = jnp.zeros((beams, LANES), jnp.float32)
                totals = lax.fori_loop(
                    0, frames // unroll, some_frames, (zero,) * (4 * polars * polars)
                )
                for x in range(2):
                    for p in range(polars):
                        low = pl.multiple_of(
                            (p * halves + half) * (polars * beams), polars * beams
                        )
                        for o in range(2):
                            value = jnp.concatenate(
                                [
                                    totals[((x * polars + p) * polars + q) * 2 + o]
                                    for q in range(polars)
                                ],
                                axis=0,
                            )
                            stage[
                                slot, o, t, pl.ds(low, polars * beams),
                                x * LANES : (x + 1) * LANES,
                            ] = value.astype(jnp.bfloat16)
                return inner_carry

            lax.fori_loop(0, (own // 2) * halves, pair, 0)
            out_copy(slot, c, s, block).start()
            return carry

        lax.fori_loop(0, own, station, 0)

    def order(step):
        if step == 0:
            return me
        two_sided = jnp.minimum(me, n - 1 - me)
        way = jnp.where(low_side, 1, -1)
        near = (step + 1) // 2
        near_block = me - way * near if step % 2 else me + way * near
        far_block = me + way * (step - two_sided)
        return jnp.where(step <= 2 * two_sided, near_block, far_block)

    def unit(c, step):
        if step == 0:
            widen(me, c, left)
        else:
            for p in range(polars):
                arrive(step, c * polars + p)
        correlate(c, order(step), c == 0 and step == 0)

    last = coarse - 1
    hops = range(1, n - 1)
    ps = range(polars)

    def take_near(c, p):
        for distance in hops:
            receive(outward, distance, c * polars + p)

    def give_near(c, p):
        for distance in hops:
            launch(outward, distance, c * polars + p)

    def pass_far(c, p, distances):
        for distance in distances:
            receive(inward_end, distance, c * polars + p)
            launch(inward_end, distance, c * polars + p)

    for p in ps:
        chunk_work(p)
    unit(0, 0)
    for c in range(1, coarse):
        prev = c - 1
        for p in ps:
            chunk_work(c * polars + p)
            launch(outward, 0, prev * polars + p)
        if c == last:
            power_start()
        for p in ps:
            take_near(prev, p)
        unit(prev, 1)
        for p in ps:
            give_near(prev, p)
            pass_far(prev, p, hops[:1])
        if c == last:
            power_finish()
        if n > 2:
            unit(prev, 2)
        for p in ps:
            if c == last:
                launch(outward, 0, last * polars + p)
            pass_far(prev, p, hops[1:])
        for step in range(3, n):
            unit(prev, step)
        if c < last:
            unit(c, 0)
    if coarse == 1:
        power_start()
        for p in ps:
            launch(outward, 0, p)
        power_finish()
    for p in ps:
        take_near(last, p)
        give_near(last, p)
        pass_far(last, p, hops[:1])
    if coarse > 1:
        unit(last, 0)
    for p in ps:
        pass_far(last, p, hops[1:])
        if p == 0 and n > 2:
            unit(last, 1)
    for step in range(1 if n == 2 else 2, n):
        if step == n - 1:
            scale_rows()
        unit(last, step)
    drain(outward)
    drain(inward_end)
    for copy in row_copies():
        copy.wait()

    for slot in range(2):
        out_copy(slot, last, own - 2 + slot, order(n - 1)).wait()
    for k in range(1, n):
        steer_copy(k).wait_send()
        scale_copy(k).wait_send()
        for chunk in range(chunks):
            dish_copy(chunk, k).wait_send()
    for k in range(1, n_chan):
        power_copy(k).wait_send()

    @pl.when(tm < n_tm - 1)
    def _():
        for chunk in range(chunks):
            halo(chunk).wait_send()

    for chunk in range(chunks):
        @pl.when(me == 0)
        def _():
            beam_copy(me, chunk, True, 0).wait_send()

        @pl.when(me == n - 1)
        def _():
            beam_copy(me, chunk, False, 0).wait_send()


def chain(volts, perm, steer, fir_taps, table, beams):
    coarse, polars, frames, _, dishes, fine = volts.shape
    n, _, terms, rows = steer.shape
    n_chan = lax.axis_size("chan")
    share = dishes // n
    chunks = coarse * polars
    half_rows = rows // 2
    own = half_rows // beams
    out_rows = beams * polars * polars * (fine // LANES)
    history = fir_taps.shape[0] - 1
    dma = pltpu.SemaphoreType.DMA
    bf16, f32 = jnp.bfloat16, jnp.float32
    size = 2 * coarse * own * n * own * out_rows * LANES
    vmem = pl.BlockSpec(memory_space=pltpu.VMEM)
    return pl.pallas_call(
        functools.partial(chain_kernel, beams),
        in_specs=[pl.BlockSpec(memory_space=pl.ANY), vmem, vmem, vmem, vmem],
        out_specs=[pl.BlockSpec(memory_space=pl.ANY)] * 3,
        out_shape=[
            jax.ShapeDtypeStruct((2, coarse, own, n * own // 2, out_rows, 2 * LANES), bf16),
            jax.ShapeDtypeStruct((own, out_rows, LANES), f32),
            jax.ShapeDtypeStruct((n * own, out_rows, LANES), f32),
        ],
        scratch_shapes=[
            pltpu.VMEM((2, frames, 2, dishes, fine), bf16),
            pltpu.VMEM((chunks, n, frames, 2, share, fine), bf16),
            pltpu.VMEM((chunks, n, frames, 2, share, fine), bf16),
            pltpu.VMEM((n, coarse, terms, rows), bf16),
            pltpu.VMEM((coarse, rows, n * terms), bf16),
            pltpu.VMEM((chunks, history + frames, rows, fine), bf16),
            pltpu.VMEM((4 * half_rows, 2 * fine), bf16),
            pltpu.VMEM((n, chunks, frames, rows, fine), bf16),
            pltpu.VMEM((polars, half_rows, fine), f32),
            pltpu.VMEM((n_chan, polars, half_rows, LANES), f32),
            pltpu.VMEM((n, polars, half_rows, LANES), f32),
            pltpu.VMEM((own, out_rows, LANES), f32),
            pltpu.VMEM((n * own, out_rows, LANES), f32),
            pltpu.VMEM((polars, frames, rows, fine), f32),
            pltpu.VMEM((polars, frames, rows, fine), f32),
            pltpu.VMEM((2, 2, own // 2, out_rows, 2 * LANES), bf16),
            dma((2,)),
            dma((chunks, n - 1)),
            dma((chunks, n - 1)),
            dma((n - 1,)),
            dma((n - 1,)),
            dma((chunks,)),
            dma((chunks,)),
            dma((2, n - 1, chunks)),
            dma((2, n - 1, chunks)),
            dma((n_chan - 1,)),
            dma((n_chan - 1,)),
            dma((n - 1,)),
            dma((n - 1,)),
            dma((2,)),
            dma((2,)),
        ],
        compiler_params=pltpu.CompilerParams(
            vmem_limit_bytes=VMEM_LIMIT, collective_id=0, has_side_effects=True
        ),
        cost_estimate=pl.CostEstimate(
            flops=size * 4 * frames * 100, bytes_accessed=size * 4, transcendentals=0
        ),
        name="chain",
    )(volts, perm, steer, fir_taps, table)


def scaling_kernel(x_ref, order_ref, left_ref, right_ref, out_ref):
    _, _, stations, pairs, rows, lanes = x_ref.shape
    group = order_ref.shape[0] // rows

    def station(s, carry):
        left = left_ref[s]
        for i in range(pairs // group):
            block = x_ref[0, 0, s, i * group : (i + 1) * group].reshape(group * rows, lanes)
            values = jnp.dot(order_ref[...], block, preferred_element_type=jnp.float32)
            for g in range(group):
                for x in range(2):
                    t = (i * group + g) * 2 + x
                    value = values[g * rows : (g + 1) * rows, x * LANES : (x + 1) * LANES]
                    out_ref[0, 0, s, t] = value * (left * right_ref[t])
        return carry

    lax.fori_loop(0, stations, station, 0)


def scaled(values, order, lrows, rrows):
    parts, coarse, own, pairs, rows, lanes = values.shape
    shape = (parts, coarse, own, 2 * pairs, rows, LANES)
    some = own // 2
    return pl.pallas_call(
        scaling_kernel,
        grid=(parts, coarse, own // some),
        in_specs=[
            pl.BlockSpec((1, 1, some, pairs, rows, lanes), lambda o, c, s: (o, c, s, 0, 0, 0)),
            pl.BlockSpec(order.shape, lambda o, c, s: (0, 0)),
            pl.BlockSpec((some, rows, LANES), lambda o, c, s: (s, 0, 0)),
            pl.BlockSpec(rrows.shape, lambda o, c, s: (0, 0, 0)),
        ],
        out_specs=pl.BlockSpec(
            (1, 1, some, 2 * pairs, rows, LANES), lambda o, c, s: (o, c, s, 0, 0, 0)
        ),
        out_shape=jax.ShapeDtypeStruct(shape, jnp.float32),
        compiler_params=pltpu.CompilerParams(vmem_limit_bytes=VMEM_LIMIT),
        cost_estimate=pl.CostEstimate(
            flops=values.size * 2 * rows, bytes_accessed=values.size * 6, transcendentals=0
        ),
        name="scaled",
    )(values, order, lrows, rrows)


def per_device(voltages, fir_taps, station_map, beam_index, weight_table):
    _, coarse_dev, dishes, frames, polars, fine = voltages.shape
    table_rows, beams = weight_table.shape[1], weight_table.shape[3]
    n = lax.axis_size("stn")
    share = dishes // n
    total_stations = 32
    own = total_stations // n
    order = jnp.arange(dishes, dtype=jnp.int32)
    block = station_map // own
    same = block[:, None] == block[None, :]
    before = order[None, :] < order[:, None]
    rank = jnp.sum((same & before).astype(jnp.int32), axis=1)
    place = block * share + rank
    hot = place[None, :] == order[:, None]
    perm = hot.astype(jnp.bfloat16)
    station = jnp.sum(jnp.where(hot, (station_map - block * own)[None, :], 0), axis=1)
    row = jnp.sum(jnp.where(hot, beam_index[None, :], 0), axis=1)
    station_hot = station[:, None] == jnp.arange(own, dtype=jnp.int32)
    table_hot = (row[:, None] == jnp.arange(table_rows, dtype=jnp.int32)).astype(jnp.bfloat16)
    weights = jnp.einsum(
        "dt,otcb->ocdb", table_hot, weight_table, preferred_element_type=jnp.float32
    ).astype(jnp.bfloat16)
    mixing = jnp.stack(
        [jnp.stack([weights[0], weights[1]]), jnp.stack([-weights[1], weights[0]])]
    )
    mixing = mixing.reshape(2, 2, coarse_dev, n, share, 1, beams)
    steer = jnp.where(
        station_hot.reshape(1, 1, 1, n, share, own, 1), mixing, jnp.zeros((), jnp.bfloat16)
    )
    steer = jnp.transpose(steer, (3, 2, 0, 4, 1, 5, 6))
    steer = steer.reshape(n, coarse_dev, 2 * share, 2 * own * beams)
    volts = jnp.transpose(voltages, (1, 4, 3, 0, 2, 5))
    halves = fine // LANES
    count = beams * polars * polars * halves
    final = np.arange(count)
    source = final % (count // beams) * beams + final // (count // beams)
    ordering = np.kron(np.eye(2), source[:, None] == final[None, :])
    ordering = jnp.asarray(ordering, jnp.bfloat16)
    result, lrows, rrows = chain(volts, perm, steer, fir_taps, dft_table(fine), beams)
    result = scaled(result, ordering, lrows, rrows)
    result = result.reshape(
        2, coarse_dev, own, total_stations, beams, polars, halves, polars, LANES
    )
    result = jnp.swapaxes(result, 6, 7)
    return result.reshape(1, 2, coarse_dev, own, total_stations, beams, polars, polars, fine)


def solution(mesh):
    in_specs = (
        P(None, "chan", "stn", "tm", None, None),
        P(),
        P("stn"),
        P("stn"),
        P(None, None, "chan", None),
    )
    out_specs = P("tm", None, "chan", "stn", None, None, None, None, None)
    return jax.shard_map(
        per_device, mesh=mesh, in_specs=in_specs, out_specs=out_specs, check_vma=False
    )
```

```python
import functools

import jax
import jax.numpy as jnp
import numpy as np
from jax import lax
from jax.experimental import pallas as pl
from jax.experimental.pallas import tpu as pltpu
from jax.sharding import PartitionSpec as P

LANES = 128
VMEM_LIMIT = 63 * 1024 * 1024
MESH = pl.DeviceIdType.MESH

epsilon = 1e-06


def dft_table(length):
    bin_index = np.arange(length)
    phase_step = bin_index[:, None] * bin_index[None, :] % length
    angles = (2.0 * np.pi / length) * phase_step
    cosine = np.cos(angles)
    sine = np.sin(angles)
    table = np.block([[cosine, -sine], [sine, cosine]])
    return jnp.asarray(table.astype(np.float32), jnp.bfloat16)


def chain_kernel(
    beams, volts, perm, steer, taps, dft, out, lout, rout,
    xin, send, recv, srecv, sfull, ybuf, fil, gbuf, pacc, pwx, scales, lrows, rrows, left, right, stage,
    relay, srelay, srelay_full, part,
    load_sem, a_send, a_recv, s_send, s_recv, h_send, h_recv,
    b_send, b_recv, p_send, p_recv, c_send, c_recv, o_sem, r_sem, q_send, q_recv, t_send, t_recv, v_send, v_recv,
):
    coarse, polars, frames, _, dishes, fine = volts.shape
    chunks = coarse * polars
    n_taps = taps.shape[0]
    history = n_taps - 1
    n = lax.axis_size("stn")
    n_tm = lax.axis_size("tm")
    n_chan = lax.axis_size("chan")
    me = lax.axis_index("stn")
    tm = lax.axis_index("tm")
    ch = lax.axis_index("chan")
    share = dishes // n
    rows = sfull.shape[1]
    half_rows = rows // 2
    own = half_rows // beams
    halves = fine // LANES
    group = 4
    unroll = 8
    ahead = 2
    base = polars if coarse > 1 and n > 3 else chunks
    ends = ((True, 0, 1), (False, n - 1, n - 2))

    barrier = pltpu.get_barrier_semaphore()
    for k in range(1, n):
        pl.semaphore_signal(
            barrier, inc=1, device_id={"stn": lax.rem(me + k, n)}, device_id_type=MESH
        )
    for k in range(1, n_chan):
        pl.semaphore_signal(
            barrier, inc=1, device_id={"chan": lax.rem(ch + k, n_chan)}, device_id_type=MESH
        )
    for k in range(1, n_tm):
        pl.semaphore_signal(
            barrier, inc=1, device_id={"tm": lax.rem(tm + k, n_tm)}, device_id_type=MESH
        )

    def load(chunk):
        return pltpu.make_async_copy(
            volts.at[chunk // polars, chunk % polars],
            xin.at[chunk % 2],
            load_sem.at[chunk % 2],
        )

    def steer_copy(k):
        dest = lax.rem(me + k, n)
        return pltpu.make_async_remote_copy(
            src_ref=steer.at[dest], dst_ref=srecv.at[me],
            send_sem=s_send.at[k - 1], recv_sem=s_recv.at[k - 1],
            device_id={"stn": dest}, device_id_type=MESH,
        )

    def steer_arrival(k):
        return pltpu.make_async_remote_copy(
            src_ref=steer.at[me], dst_ref=srecv.at[lax.rem(me + n - k, n)],
            send_sem=s_send.at[k - 1], recv_sem=s_recv.at[k - 1],
            device_id={"stn": lax.rem(me + k, n)}, device_id_type=MESH,
        )

    def dish_copy(chunk, k):
        dest = lax.rem(me + k, n)
        return pltpu.make_async_remote_copy(
            src_ref=send.at[chunk, dest], dst_ref=recv.at[chunk, me],
            send_sem=a_send.at[chunk, k - 1], recv_sem=a_recv.at[chunk, k - 1],
            device_id={"stn": dest}, device_id_type=MESH,
        )

    def dish_arrival(chunk, k):
        return pltpu.make_async_remote_copy(
            src_ref=send.at[chunk, me], dst_ref=recv.at[chunk, lax.rem(me + n - k, n)],
            send_sem=a_send.at[chunk, k - 1], recv_sem=a_recv.at[chunk, k - 1],
            device_id={"stn": lax.rem(me + k, n)}, device_id_type=MESH,
        )

    def relay_copy(chunk, low, end, target):
        slot = me - 1 if low else me
        return pltpu.make_async_remote_copy(
            src_ref=send.at[chunk, end], dst_ref=relay.at[chunk - base, slot],
            send_sem=q_send.at[chunk - base, int(low)], recv_sem=q_recv.at[chunk - base, slot],
            device_id={"stn": jnp.int32(target)}, device_id_type=MESH,
        )

    def relay_arrival(chunk, slot):
        return pltpu.make_async_remote_copy(
            src_ref=send.at[chunk, me], dst_ref=relay.at[chunk - base, slot],
            send_sem=q_send.at[chunk - base, 0], recv_sem=q_recv.at[chunk - base, slot],
            device_id={"stn": lax.rem(me + 1, n)}, device_id_type=MESH,
        )

    def steer_relay(low, end, target):
        slot = me - 1 if low else me
        return pltpu.make_async_remote_copy(
            src_ref=steer.at[end], dst_ref=srelay.at[slot],
            send_sem=t_send.at[int(low)], recv_sem=t_recv.at[slot],
            device_id={"stn": jnp.int32(target)}, device_id_type=MESH,
        )

    def steer_relay_arrival(slot):
        return pltpu.make_async_remote_copy(
            src_ref=steer.at[me], dst_ref=srelay.at[slot],
            send_sem=t_send.at[0], recv_sem=t_recv.at[slot],
            device_id={"stn": lax.rem(me + 1, n)}, device_id_type=MESH,
        )

    def part_copy(chunk, end):
        return pltpu.make_async_remote_copy(
            src_ref=part.at[chunk - base], dst_ref=part.at[chunk - base],
            send_sem=v_send.at[chunk - base], recv_sem=v_recv.at[chunk - base],
            device_id={"stn": jnp.int32(end)}, device_id_type=MESH,
        )

    def past_neighbour(low):
        return me >= 2 if low else me <= n - 3

    at_end = jnp.logical_or(me == 0, me == n - 1)

    def send_dishes(chunk):
        for distance in range(1, n):
            @pl.when(me + distance < (n if chunk < base else n - 1))
            def _():
                dish_copy(chunk, distance).start()

            @pl.when(me - distance >= (0 if chunk < base else 1))
            def _():
                dish_copy(chunk, n - distance).start()

        if chunk >= base:
            for low, end, target in ends:
                @pl.when(past_neighbour(low))
                def _():
                    relay_copy(chunk, low, end, target).start()

    load(0).start()
    srecv[me] = steer[me]

    for chunk in range(chunks):
        load(chunk).wait()
        if chunk + 1 < chunks:
            load(chunk + 1).start()

        def sort_step(i, carry):
            frame = i // 2
            o = i % 2
            moved = jnp.dot(
                perm[...], xin[chunk % 2, frame, o], preferred_element_type=jnp.float32
            ).astype(jnp.bfloat16)
            for dest in range(n):
                send[chunk, dest, frame, o] = moved[dest * share : (dest + 1) * share]
            return carry

        lax.fori_loop(0, 2 * frames, sort_step, 0)
        if chunk == 0:
            pl.semaphore_wait(barrier, (n - 1) + (n_chan - 1) + (n_tm - 1))
            for k in range(1, n):
                steer_copy(k).start()
            if base < chunks:
                for low, end, target in ends:
                    @pl.when(past_neighbour(low))
                    def _():
                        steer_relay(low, end, target).start()
        if chunk < ahead:
            send_dishes(chunk)

    def keep_step(i, carry):
        for chunk in range(chunks):
            recv[chunk, me, i] = send[chunk, me, i]
        return carry

    lax.fori_loop(0, frames, keep_step, 0)

    @pl.when(tm == 0)
    def _():
        def zero_step(i, carry):
            for chunk in range(chunks):
                ybuf[chunk, i] = jnp.zeros((rows, fine), jnp.bfloat16)
            return carry

        lax.fori_loop(0, history, zero_step, 0)

    pacc[...] = jnp.zeros_like(pacc)

    for k in range(1, n):
        steer_arrival(k).wait_recv()
    for c in range(coarse):
        columns = srecv[:, c].astype(jnp.float32).reshape(n * 2 * share, rows)
        sfull[c] = jnp.transpose(columns).astype(jnp.bfloat16)

    def prepare_relay(low, end, target):
        mine = 0 if low else n - 2
        srelay[mine] = steer[end]
        for slot in range(n - 1):
            if slot != mine:
                steer_relay_arrival(slot).wait_recv()
        for c in range(1, coarse):
            columns = srelay[:, c].astype(jnp.float32).reshape((n - 1) * 2 * share, rows)
            srelay_full[c - 1] = jnp.transpose(columns).astype(jnp.bfloat16)

        def own_step(i, carry):
            for chunk in range(base, chunks):
                relay[chunk - base, mine, i] = send[chunk, end, i]
            return carry

        lax.fori_loop(0, frames, own_step, 0)

    def relay_work(chunk, low, end):
        mine = 0 if low else n - 2
        for slot in range(n - 1):
            if slot != mine:
                relay_arrival(chunk, slot).wait_recv()

        def relay_step(frame, carry):
            terms = relay[chunk - base, :, frame].reshape(-1, fine)
            total = jnp.dot(
                srelay_full[chunk // polars - 1], terms, preferred_element_type=jnp.float32
            )
            part[chunk - base, frame] = total.astype(jnp.bfloat16)
            return carry

        lax.fori_loop(0, frames, relay_step, 0)
        part_copy(chunk, end).start()

    if base < chunks:
        for low, end, target in ends:
            @pl.when(me == target)
            def _():
                prepare_relay(low, end, target)

        @pl.when(at_end)
        def _():
            def blank_step(i, carry):
                for chunk in range(base, chunks):
                    for k in range(1, n):
                        recv[chunk, lax.rem(me + k, n), i] = jnp.zeros(
                            (2, share, fine), jnp.bfloat16
                        )
                return carry

            lax.fori_loop(0, frames, blank_step, 0)

    def halo(chunk):
        return pltpu.make_async_remote_copy(
            src_ref=ybuf.at[chunk, pl.ds(frames, history)],
            dst_ref=ybuf.at[chunk, pl.ds(0, history)],
            send_sem=h_send.at[chunk], recv_sem=h_recv.at[chunk],
            device_id={"tm": lax.rem(tm + 1, n_tm)}, device_id_type=MESH,
        )

    def beam_copy(block, chunk, right_way, distance):
        target = me + 1 if right_way else me - 1
        way = 0 if right_way else 1
        return pltpu.make_async_remote_copy(
            src_ref=gbuf.at[block, chunk], dst_ref=gbuf.at[block, chunk],
            send_sem=b_send.at[way, distance, chunk], recv_sem=b_recv.at[way, distance, chunk],
            device_id={"stn": lax.rem(target + n, n)}, device_id_type=MESH,
        )

    inner = jnp.logical_and(me > 0, me < n - 1)
    low_side = me < n - 1 - me

    def on_side(far_way, distance, chunk, hop, act):
        for right_way in (True, False):
            block = me - distance if right_way else me + distance
            inside = block >= 0 if right_way else block < n
            side = low_side if right_way == far_way else jnp.logical_not(low_side)

            @pl.when(jnp.logical_and(jnp.logical_and(inner, side), inside))
            def _():
                act(beam_copy(block, chunk, right_way, hop))

    outward = (True, 2, [])
    inward_end = (False, 5, [])

    def launch(queue, distance, chunk):
        far_way, window, started = queue
        if len(started) >= window:
            past, past_chunk = started[-window]
            on_side(far_way, past, past_chunk, past, lambda copy: copy.wait_send())
        started.append((distance, chunk))
        on_side(far_way, distance, chunk, distance, lambda copy: copy.start())

    def receive(queue, distance, chunk):
        on_side(queue[0], distance, chunk, distance - 1, lambda copy: copy.wait_recv())

    def drain(queue):
        far_way, window, started = queue
        for distance, chunk in started[-window:]:
            on_side(far_way, distance, chunk, distance, lambda copy: copy.wait_send())

    def chunk_work(chunk):
        c, p = chunk // polars, chunk % polars
        relayed = chunk >= base

        def arrivals():
            for k in range(1, n):
                dish_arrival(chunk, k).wait_recv()

        if relayed:
            pl.when(jnp.logical_not(at_end))(arrivals)
        else:
            arrivals()
        if chunk + ahead < chunks:
            send_dishes(chunk + ahead)

        def beam_step(frame, carry):
            terms = recv[chunk, :, frame]
            if share % 16:
                terms = terms.astype(jnp.float32).reshape(-1, fine).astype(jnp.bfloat16)
            else:
                terms = terms.reshape(-1, fine)
            formed = jnp.dot(sfull[c], terms, preferred_element_type=jnp.float32)
            ybuf[chunk, history + frame] = formed.astype(jnp.bfloat16)
            return carry

        def end_step(frame, carry):
            terms = recv[chunk, :, frame].reshape(-1, fine)
            formed = jnp.dot(sfull[c], terms, preferred_element_type=jnp.float32)
            formed = formed + part[chunk - base, frame].astype(jnp.float32)
            ybuf[chunk, history + frame] = formed.astype(jnp.bfloat16)
            return carry

        if relayed:
            @pl.when(at_end)
            def _():
                part_copy(chunk, 0).wait_recv()
                lax.fori_loop(0, frames, end_step, 0)

            @pl.when(jnp.logical_not(at_end))
            def _():
                lax.fori_loop(0, frames, beam_step, 0)

        else:
            lax.fori_loop(0, frames, beam_step, 0)

        @pl.when(tm < n_tm - 1)
        def _():
            halo(chunk).start()

        @pl.when(tm > 0)
        def _():
            halo(chunk).wait_recv()

        band = min(32, half_rows)

        def filter_step(i, carry):
            for j in range(group):
                frame = i * group + j
                for o in range(2):
                    for low in range(0, half_rows, band):
                        start = o * half_rows + low
                        total = jnp.zeros((band, fine), jnp.float32)
                        for tap in range(n_taps):
                            sample = ybuf[chunk, frame + (history - tap), start : start + band, :]
                            total = total + taps[tap : tap + 1, :] * sample.astype(jnp.float32)
                        fil[
                            j * half_rows + low : j * half_rows + low + band,
                            o * fine : (o + 1) * fine,
                        ] = total.astype(jnp.bfloat16)
            spec = jnp.dot(fil[...], dft[...], preferred_element_type=jnp.float32)
            spec = spec.astype(jnp.bfloat16)
            for j in range(group):
                for o in range(2):
                    values = spec[j * half_rows : (j + 1) * half_rows, o * fine : (o + 1) * fine]
                    gbuf[me, chunk, i * group + j, o * half_rows : (o + 1) * half_rows, :] = values
                    wide = values.astype(jnp.float32)
                    pacc[p] += wide * wide
            return carry

        lax.fori_loop(0, frames // group, filter_step, 0)

        @pl.when(me == 0)
        def _():
            beam_copy(me, chunk, True, 0).start()

        @pl.when(me == n - 1)
        def _():
            beam_copy(me, chunk, False, 0).start()

        launch(inward_end, 0, chunk)
        if relayed:
            for low, end, target in ends:
                @pl.when(me == target)
                def _():
                    relay_work(chunk, low, end)

    def arrive(distance, chunk):
        @pl.when(me == n - 1)
        def _():
            beam_copy(me - distance, chunk, True, distance - 1).wait_recv()

        @pl.when(me == 0)
        def _():
            beam_copy(me + distance, chunk, False, distance - 1).wait_recv()

    def power_copy(k):
        return pltpu.make_async_remote_copy(
            src_ref=pwx.at[ch], dst_ref=pwx.at[ch],
            send_sem=p_send.at[k - 1], recv_sem=p_recv.at[k - 1],
            device_id={"chan": lax.rem(ch + k, n_chan)}, device_id_type=MESH,
        )

    def power_arrival(k):
        other = lax.rem(ch + n_chan - k, n_chan)
        return pltpu.make_async_remote_copy(
            src_ref=pwx.at[ch], dst_ref=pwx.at[other],
            send_sem=p_send.at[k - 1], recv_sem=p_recv.at[k - 1],
            device_id={"chan": lax.rem(ch + k, n_chan)}, device_id_type=MESH,
        )

    def scale_copy(k):
        return pltpu.make_async_remote_copy(
            src_ref=scales.at[me], dst_ref=scales.at[me],
            send_sem=c_send.at[k - 1], recv_sem=c_recv.at[k - 1],
            device_id={"stn": lax.rem(me + k, n)}, device_id_type=MESH,
        )

    def scale_arrival(k):
        other = lax.rem(me + n - k, n)
        return pltpu.make_async_remote_copy(
            src_ref=scales.at[me], dst_ref=scales.at[other],
            send_sem=c_send.at[k - 1], recv_sem=c_recv.at[k - 1],
            device_id={"stn": lax.rem(me + k, n)}, device_id_type=MESH,
        )

    def power_start():
        for p in range(polars):
            total = jnp.sum(pacc[p], axis=1, keepdims=True)
            pwx[ch, p] = jnp.broadcast_to(total, (half_rows, LANES))
        for k in range(1, n_chan):
            power_copy(k).start()

    def power_finish():
        for k in range(1, n_chan):
            power_arrival(k).wait_recv()
        total = pwx[0]
        for k in range(1, n_chan):
            total = total + pwx[k]
        scales[me] = lax.rsqrt(total / (coarse * n_chan * frames * fine) + epsilon)
        for k in range(1, n):
            scale_copy(k).start()

    def row_copies():
        return (
            pltpu.make_async_copy(lrows, lout, r_sem.at[0]),
            pltpu.make_async_copy(rrows, rout, r_sem.at[1]),
        )

    def scale_rows():
        for k in range(1, n):
            scale_arrival(k).wait_recv()

        def spread(t, target, by_left, block):
            row = pl.multiple_of(lax.rem(t, own) * beams, beams)
            for p in range(polars):
                for half in range(halves):
                    for q in range(polars):
                        where = pl.ds(
                            (p * halves + half) * polars + q, beams,
                            stride=polars * polars * halves,
                        )
                        value = scales[block, p if by_left else q, pl.ds(row, beams), :]
                        target[t, where, :] = value * (1.0 / frames) if by_left else value

        def left_step(t, carry):
            spread(t, lrows, True, me)
            return carry

        def right_step(t, carry):
            spread(t, rrows, False, t // own)
            return carry

        lax.fori_loop(0, own, left_step, 0)
        lax.fori_loop(0, n * own, right_step, 0)
        for copy in row_copies():
            copy.start()

    def widen(block, c, target):
        def step(i, carry):
            for p in range(polars):
                target[p, i] = gbuf[block, c * polars + p, i].astype(jnp.float32)
            return carry

        lax.fori_loop(0, frames, step, 0)

    def out_copy(slot, c, s, block):
        return pltpu.make_async_copy(
            stage.at[slot], out.at[:, c, s, pl.ds(block * (own // 2), own // 2)], o_sem.at[slot]
        )

    def correlate(c, block, first):
        widen(block, c, right)

        def station(s, carry):
            slot = s % 2
            srow = pl.multiple_of(s * beams, beams)
            if first:
                @pl.when(s >= 2)
                def _():
                    out_copy(slot, c, s, block).wait()
            else:
                out_copy(slot, c, s, block).wait()

            def pair(i, inner_carry):
                half = i % halves
                t = i // halves
                lanes = pl.ds(pl.multiple_of(half * LANES, LANES), LANES)
                trows = [pl.multiple_of((2 * t + x) * beams, beams) for x in range(2)]

                def some_frames(k, totals):
                    totals = list(totals)
                    for j in range(unroll):
                        f = k * unroll + j
                        lre = [left[p, f, pl.ds(srow, beams), lanes] for p in range(polars)]
                        lim = [
                            left[p, f, pl.ds(half_rows + srow, beams), lanes]
                            for p in range(polars)
                        ]
                        for x in range(2):
                            rre = [
                                right[q, f, pl.ds(trows[x], beams), lanes] for q in range(polars)
                            ]
                            rim = [
                                right[q, f, pl.ds(half_rows + trows[x], beams), lanes]
                                for q in range(polars)
                            ]
                            for p in range(polars):
                                for q in range(polars):
                                    at = ((x * polars + p) * polars + q) * 2
                                    totals[at] += lre[p] * rre[q] + lim[p] * rim[q]
                                    totals[at + 1] += lim[p] * rre[q] - lre[p] * rim[q]
                    return tuple(totals)

                zero = jnp.zeros((beams, LANES), jnp.float32)
                totals = lax.fori_loop(
                    0, frames // unroll, some_frames, (zero,) * (4 * polars * polars)
                )
                for x in range(2):
                    for p in range(polars):
                        low = pl.multiple_of(
                            (p * halves + half) * (polars * beams), polars * beams
                        )
                        for o in range(2):
                            value = jnp.concatenate(
                                [
                                    totals[((x * polars + p) * polars + q) * 2 + o]
                                    for q in range(polars)
                                ],
                                axis=0,
                            )
                            stage[
                                slot, o, t, pl.ds(low, polars * beams),
                                x * LANES : (x + 1) * LANES,
                            ] = value.astype(jnp.bfloat16)
                return inner_carry

            lax.fori_loop(0, (own // 2) * halves, pair, 0)
            out_copy(slot, c, s, block).start()
            return carry

        lax.fori_loop(0, own, station, 0)

    def order(step):
        if step == 0:
            return me
        two_sided = jnp.minimum(me, n - 1 - me)
        way = jnp.where(low_side, 1, -1)
        near = (step + 1) // 2
        near_block = me - way * near if step % 2 else me + way * near
        far_block = me + way * (step - two_sided)
        return jnp.where(step <= 2 * two_sided, near_block, far_block)

    wide_of = []

    def unit(c, step):
        if wide_of[-1:] != [c]:
            widen(me, c, left)
            wide_of.append(c)
        if step:
            for p in range(polars):
                arrive(step, c * polars + p)
        correlate(c, order(step), c == 0 and step == 0)

    last = coarse - 1
    hops = range(1, n - 1)
    ps = range(polars)

    def take_near(c, p):
        for distance in hops:
            receive(outward, distance, c * polars + p)

    def give_near(c, p):
        for distance in hops:
            launch(outward, distance, c * polars + p)

    def pass_far(c, p, distances):
        for distance in distances:
            receive(inward_end, distance, c * polars + p)
            launch(inward_end, distance, c * polars + p)

    for p in ps:
        chunk_work(p)
    unit(0, 0)
    for c in range(1, coarse):
        prev = c - 1
        for p in ps:
            chunk_work(c * polars + p)
            launch(outward, 0, prev * polars + p)
        if c == last:
            power_start()
        for p in ps:
            take_near(prev, p)
        unit(prev, 1)
        for p in ps:
            if c == last:
                launch(outward, 0, last * polars + p)
            pass_far(prev, p, hops[:1])
        if c == last:
            power_finish()
        if n > 2:
            unit(prev, 2)
        if c < last:
            for p in ps:
                give_near(prev, p)
                pass_far(prev, p, hops[1:])
            for step in range(3, n):
                unit(prev, step)
            unit(c, 0)
    prev = last - 1
    if coarse == 1:
        power_start()
        power_finish()
        for p in ps:
            launch(outward, 0, p)
            take_near(last, p)
            give_near(last, p)
            pass_far(last, p, hops)
        for step in range(1, n - 1):
            unit(last, step)
    else:
        for p in ps:
            give_near(prev, p)
            pass_far(last, p, hops[:1])
            if p < n - 1:
                unit(last, p)
            if p == 0:
                for q in ps:
                    take_near(last, q)
        for p in ps:
            give_near(last, p)
            pass_far(prev, p, hops[1:])
            if p == 0:
                for step in range(polars, n - 1):
                    unit(last, step)
        pass_far(last, 0, hops[1:])
        for step in range(3, n):
            unit(prev, step)
        for p in ps[1:]:
            pass_far(last, p, hops[1:])
    scale_rows()
    unit(last, n - 1)
    drain(outward)
    drain(inward_end)
    for copy in row_copies():
        copy.wait()

    for slot in range(2):
        out_copy(slot, last, own - 2 + slot, order(n - 1)).wait()
    for k in range(1, n):
        steer_copy(k).wait_send()
        scale_copy(k).wait_send()
        to_end = jnp.logical_or(lax.rem(me + k, n) == 0, lax.rem(me + k, n) == n - 1)
        for chunk in range(base):
            dish_copy(chunk, k).wait_send()
        for chunk in range(base, chunks):
            @pl.when(jnp.logical_not(to_end))
            def _():
                dish_copy(chunk, k).wait_send()
    for k in range(1, n_chan):
        power_copy(k).wait_send()
    if base < chunks:
        for low, end, target in ends:
            @pl.when(past_neighbour(low))
            def _():
                steer_relay(low, end, target).wait_send()
                for chunk in range(base, chunks):
                    relay_copy(chunk, low, end, target).wait_send()

            @pl.when(me == target)
            def _():
                for chunk in range(base, chunks):
                    part_copy(chunk, end).wait_send()

    @pl.when(tm < n_tm - 1)
    def _():
        for chunk in range(chunks):
            halo(chunk).wait_send()

    for chunk in range(chunks):
        @pl.when(me == 0)
        def _():
            beam_copy(me, chunk, True, 0).wait_send()

        @pl.when(me == n - 1)
        def _():
            beam_copy(me, chunk, False, 0).wait_send()


def chain(volts, perm, steer, fir_taps, table, beams):
    coarse, polars, frames, _, dishes, fine = volts.shape
    n, _, terms, rows = steer.shape
    n_chan = lax.axis_size("chan")
    share = dishes // n
    chunks = coarse * polars
    half_rows = rows // 2
    own = half_rows // beams
    out_rows = beams * polars * polars * (fine // LANES)
    history = fir_taps.shape[0] - 1
    dma = pltpu.SemaphoreType.DMA
    late = chunks - polars if coarse > 1 and n > 3 else 1
    late_shape = (frames, 2, share, fine) if coarse > 1 and n > 3 else (1, 1, 16, fine)
    late_c = max(coarse - 1, 1)
    bf16, f32 = jnp.bfloat16, jnp.float32
    size = 2 * coarse * own * n * own * out_rows * LANES
    vmem = pl.BlockSpec(memory_space=pltpu.VMEM)
    return pl.pallas_call(
        functools.partial(chain_kernel, beams),
        in_specs=[pl.BlockSpec(memory_space=pl.ANY), vmem, vmem, vmem, vmem],
        out_specs=[pl.BlockSpec(memory_space=pl.ANY)] * 3,
        out_shape=[
            jax.ShapeDtypeStruct((2, coarse, own, n * own // 2, out_rows, 2 * LANES), bf16),
            jax.ShapeDtypeStruct((own, out_rows, LANES), f32),
            jax.ShapeDtypeStruct((n * own, out_rows, LANES), f32),
        ],
        scratch_shapes=[
            pltpu.VMEM((2, frames, 2, dishes, fine), bf16),
            pltpu.VMEM((chunks, n, frames, 2, share, fine), bf16),
            pltpu.VMEM((chunks, n, frames, 2, share, fine), bf16),
            pltpu.VMEM((n, coarse, terms, rows), bf16),
            pltpu.VMEM((coarse, rows, n * terms), bf16),
            pltpu.VMEM((chunks, history + frames, rows, fine), bf16),
            pltpu.VMEM((4 * half_rows, 2 * fine), bf16),
            pltpu.VMEM((n, chunks, frames, rows, fine), bf16),
            pltpu.VMEM((polars, half_rows, fine), f32),
            pltpu.VMEM((n_chan, polars, half_rows, LANES), f32),
            pltpu.VMEM((n, polars, half_rows, LANES), f32),
            pltpu.VMEM((own, out_rows, LANES), f32),
            pltpu.VMEM((n * own, out_rows, LANES), f32),
            pltpu.VMEM((polars, frames, rows, fine), f32),
            pltpu.VMEM((polars, frames, rows, fine), f32),
            pltpu.VMEM((2, 2, own // 2, out_rows, 2 * LANES), bf16),
            pltpu.VMEM((late, n - 1) + late_shape, bf16),
            pltpu.VMEM((n - 1, coarse, terms, rows), bf16),
            pltpu.VMEM((late_c, rows, (n - 1) * terms), bf16),
            pltpu.VMEM((late, late_shape[0], rows, fine), bf16),
            dma((2,)),
            dma((chunks, n - 1)),
            dma((chunks, n - 1)),
            dma((n - 1,)),
            dma((n - 1,)),
            dma((chunks,)),
            dma((chunks,)),
            dma((2, n - 1, chunks)),
            dma((2, n - 1, chunks)),
            dma((n_chan - 1,)),
            dma((n_chan - 1,)),
            dma((n - 1,)),
            dma((n - 1,)),
            dma((2,)),
            dma((2,)),
            dma((late, 2)),
            dma((late, n - 1)),
            dma((2,)),
            dma((n - 1,)),
            dma((late,)),
            dma((late,)),
        ],
        compiler_params=pltpu.CompilerParams(
            vmem_limit_bytes=VMEM_LIMIT, collective_id=0, has_side_effects=True
        ),
        cost_estimate=pl.CostEstimate(
            flops=size * 4 * frames * 100, bytes_accessed=size * 4, transcendentals=0
        ),
        name="chain",
    )(volts, perm, steer, fir_taps, table)


def scaling_kernel(x_ref, order_ref, left_ref, right_ref, out_ref):
    _, _, stations, pairs, rows, lanes = x_ref.shape
    group = order_ref.shape[0] // rows

    def station(s, carry):
        left = left_ref[s]
        for i in range(pairs // group):
            block = x_ref[0, 0, s, i * group : (i + 1) * group].reshape(group * rows, lanes)
            values = jnp.dot(order_ref[...], block, preferred_element_type=jnp.float32)
            for g in range(group):
                for x in range(2):
                    t = (i * group + g) * 2 + x
                    value = values[g * rows : (g + 1) * rows, x * LANES : (x + 1) * LANES]
                    out_ref[0, 0, s, t] = value * (left * right_ref[t])
        return carry

    lax.fori_loop(0, stations, station, 0)


def scaled(values, order, lrows, rrows):
    parts, coarse, own, pairs, rows, lanes = values.shape
    shape = (parts, coarse, own, 2 * pairs, rows, LANES)
    some = own // 2
    return pl.pallas_call(
        scaling_kernel,
        grid=(parts, coarse, own // some),
        in_specs=[
            pl.BlockSpec((1, 1, some, pairs, rows, lanes), lambda o, c, s: (o, c, s, 0, 0, 0)),
            pl.BlockSpec(order.shape, lambda o, c, s: (0, 0)),
            pl.BlockSpec((some, rows, LANES), lambda o, c, s: (s, 0, 0)),
            pl.BlockSpec(rrows.shape, lambda o, c, s: (0, 0, 0)),
        ],
        out_specs=pl.BlockSpec(
            (1, 1, some, 2 * pairs, rows, LANES), lambda o, c, s: (o, c, s, 0, 0, 0)
        ),
        out_shape=jax.ShapeDtypeStruct(shape, jnp.float32),
        compiler_params=pltpu.CompilerParams(vmem_limit_bytes=VMEM_LIMIT),
        cost_estimate=pl.CostEstimate(
            flops=values.size * 2 * rows, bytes_accessed=values.size * 6, transcendentals=0
        ),
        name="scaled",
    )(values, order, lrows, rrows)


def per_device(voltages, fir_taps, station_map, beam_index, weight_table):
    _, coarse_dev, dishes, frames, polars, fine = voltages.shape
    table_rows, beams = weight_table.shape[1], weight_table.shape[3]
    n = lax.axis_size("stn")
    share = dishes // n
    total_stations = 32
    own = total_stations // n
    order = jnp.arange(dishes, dtype=jnp.int32)
    block = station_map // own
    same = block[:, None] == block[None, :]
    before = order[None, :] < order[:, None]
    rank = jnp.sum((same & before).astype(jnp.int32), axis=1)
    place = block * share + rank
    hot = place[None, :] == order[:, None]
    perm = hot.astype(jnp.bfloat16)
    station = jnp.sum(jnp.where(hot, (station_map - block * own)[None, :], 0), axis=1)
    row = jnp.sum(jnp.where(hot, beam_index[None, :], 0), axis=1)
    station_hot = station[:, None] == jnp.arange(own, dtype=jnp.int32)
    table_hot = (row[:, None] == jnp.arange(table_rows, dtype=jnp.int32)).astype(jnp.bfloat16)
    weights = jnp.einsum(
        "dt,otcb->ocdb", table_hot, weight_table, preferred_element_type=jnp.float32
    ).astype(jnp.bfloat16)
    mixing = jnp.stack(
        [jnp.stack([weights[0], weights[1]]), jnp.stack([-weights[1], weights[0]])]
    )
    mixing = mixing.reshape(2, 2, coarse_dev, n, share, 1, beams)
    steer = jnp.where(
        station_hot.reshape(1, 1, 1, n, share, own, 1), mixing, jnp.zeros((), jnp.bfloat16)
    )
    steer = jnp.transpose(steer, (3, 2, 0, 4, 1, 5, 6))
    steer = steer.reshape(n, coarse_dev, 2 * share, 2 * own * beams)
    volts = jnp.transpose(voltages, (1, 4, 3, 0, 2, 5))
    halves = fine // LANES
    count = beams * polars * polars * halves
    final = np.arange(count)
    source = final % (count // beams) * beams + final // (count // beams)
    ordering = np.kron(np.eye(2), source[:, None] == final[None, :])
    ordering = jnp.asarray(ordering, jnp.bfloat16)
    result, lrows, rrows = chain(volts, perm, steer, fir_taps, dft_table(fine), beams)
    result = scaled(result, ordering, lrows, rrows)
    result = result.reshape(
        2, coarse_dev, own, total_stations, beams, polars, halves, polars, LANES
    )
    result = jnp.swapaxes(result, 6, 7)
    return result.reshape(1, 2, coarse_dev, own, total_stations, beams, polars, polars, fine)


def solution(mesh):
    in_specs = (
        P(None, "chan", "stn", "tm", None, None),
        P(),
        P("stn"),
        P("stn"),
        P(None, None, "chan", None),
    )
    out_specs = P("tm", None, "chan", "stn", None, None, None, None, None)
    return jax.shard_map(
        per_device, mesh=mesh, in_specs=in_specs, out_specs=out_specs, check_vma=False
    )
```
